256 devices in a mesh: cls: 8 (over x, y_hi), str: 32 (over z, y_lo, core).
Axes of the slice: x: 4, y: 4 (y_hi: 2, y_lo: 2; y = y_hi * 2 + y_lo), z: 8, core: 2. Of those that a mesh axis runs over, the one named last changes fastest.
Arguments:
- first_factor_tiles: float32 [8, 1024, 2, 4, 1024], P(None, ('cls', 'str')), may hold values from -6 to 6
- b_blocks: float32 [8, 1024, 2, 4, 512], P(None, ('cls', 'str')), may hold values from -0.0625 to 0.0625
Outputs:
- c_blocks: float32 [8, 1024, 2, 4, 512], P(None, ('cls', 'str'))
The draws below stay inside these ranges and needn't reach their ends.
All inputs are finite; a program needn't handle non-finite values.
Results may differ from the reference program's by a relative error of at most 0.0003.
Values sent between devices are 32-bit elements; how exact they have to be, the bound alone decides.
No kernel may reach another device: no remote copies, remote signals or barrier semaphores. Data moves between devices by JAX's collectives and lax.ppermute only.
A program may use at most 64 MiB of HBM per device.

```python
import jax
import jax.numpy as jnp
import numpy as np
from jax import lax

N = 8192
Q = 1024
QC = 512


def block_levels(key, extent, split, low, largest):
    level = 1.0
    for position, parts in split:
        draws = jax.random.uniform(jax.random.fold_in(jax.random.fold_in(key, 6), position), (parts,), jnp.float32, low / len(split), largest / len(split))
        level = level * jnp.repeat(jnp.exp(draws), extent[position] // parts).reshape((-1,) + (1,) * (len(extent) - 1 - position))
    return level


def scatter_about(key, dims, width, bound, shards=(), kind=jnp.bfloat16):
    drawn = width * jax.random.normal(key, dims, jnp.float32)
    if shards:
        drawn = drawn * block_levels(key, dims, shards, -0.22, 0.18)
    return jnp.clip(drawn, -bound, bound).astype(kind)


def setup_inputs(seed: int = 0) -> dict:
    key_of = jax.random.split(jax.random.key(seed), 3)
    return {
        "first_factor_tiles": scatter_about(key_of[0], (8, Q, 2, 4, Q), 1.0, 6.0, ((1, 256),), jnp.float32),
        "b_blocks": scatter_about(key_of[1], (8, Q, 2, 4, QC), N ** -0.5, 0.0625, ((1, 256),), jnp.float32),
    }


def strassen_weight_lists():
    left_base = np.array([[1, 0, 0, 0], [0, 1, 0, 0], [1, 1, -1, -1], [0, 0, 0, 1], [0, 0, 1, 1], [-1, 0, 1, 1], [1, 0, -1, 0]], np.float32)
    right_base_matrix = np.array([[1, 0, 0, 0], [0, 0, 1, 0], [0, 0, 0, 1], [1, -1, -1, 1], [-1, 1, 0, 0], [1, -1, 0, 1], [0, -1, 0, 1]], np.float32)
    product_grid_start = np.array([[1, 1, 0, 0, 0, 0, 0], [1, 0, 1, 0, 1, 1, 0], [1, 0, 0, -1, 0, 1, 1], [1, 0, 0, 0, 1, 1, 1]], np.float32)
    left_split = left_base.reshape(7, 2, 2)
    right_split = right_base_matrix.reshape(7, 2, 2)
    outer_split = product_grid_start.reshape(2, 2, 7)
    left_table = (left_split[:, None, :, None, :, None] * left_split[None, :, None, :, None, :]).reshape(49, 4, 4)
    right_table = (right_split[:, None, :, None, :, None] * right_split[None, :, None, :, None, :]).reshape(49, 4, 4)
    outer_table = (outer_split[:, None, :, None, :, None] * outer_split[None, :, None, :, None, :]).reshape(4, 4, 49)
    return left_table, right_table, outer_table


def reference(first_factor_tiles, b_blocks):
    first_factor_host_grid, second_factor_host_grid, product_host_grid = strassen_weight_lists()
    left_table = jnp.asarray(first_factor_host_grid).astype(first_factor_tiles.dtype)
    right_table = jnp.asarray(second_factor_host_grid).astype(first_factor_tiles.dtype)
    outer_table = jnp.asarray(product_host_grid).astype(first_factor_tiles.dtype)
    product_ids = np.arange(8)
    inner_halves = product_ids // 4
    row_half_split = (product_ids // 2) % 2
    col_halves = product_ids % 2
    a_six = first_factor_tiles.reshape(2, 4, Q, 2, 4, Q)
    b_six = b_blocks.reshape(2, 4, Q, 2, 4, QC)
    left_stack = a_six[row_half_split, :, :, inner_halves]
    right_stack = b_six[inner_halves, :, :, col_halves]
    highest = lax.Precision.HIGHEST

    def leaf_product(pair):
        x_quad, y_quad = pair
        left_leaves = jnp.einsum('mac,aqcr->mqr', left_table, x_quad, precision=highest)
        right_leaves = jnp.einsum('mac,aqcr->mqr', right_table, y_quad, precision=highest)
        leaf_out = jnp.einsum('mqk,mkr->mqr', left_leaves, right_leaves, precision=highest)
        return jnp.einsum('acm,mqr->aqcr', outer_table, leaf_out, precision=highest)

    partials = lax.map(leaf_product, (left_stack, right_stack))
    partials = partials.reshape(2, 2, 2, 4, Q, 4, QC)
    summed = partials[0] + partials[1]
    summed = jnp.transpose(summed, (0, 2, 3, 1, 4, 5))
    return summed.reshape(8, Q, 2, 4, QC)
```

```python
import jax
import jax.numpy as jnp
from jax import lax
from jax.sharding import Mesh
from jax.sharding import PartitionSpec as P

AXES = ("x", "yh", "z", "yl", "c")
Y = ("yh", "yl")


def swap(v, axis, bits):
    n = lax.axis_size(axis)
    return lax.ppermute(v, axis, [(i, i ^ bits) for i in range(n)])


def shift(v, axis, step):
    n = lax.axis_size(axis)
    return lax.ppermute(v, axis, [(i, (i + step) % n) for i in range(n)])


def pick(pieces, index):
    low = jnp.where(index % 2 == 1, pieces[1], pieces[0])
    high = jnp.where(index % 2 == 1, pieces[3], pieces[2])
    return jnp.where(index >= 2, high, low)


def lane_order(z, c):
    src = lax.broadcasted_iota(jnp.int32, (256, 256), 0)
    dst = lax.broadcasted_iota(jnp.int32, (256, 256), 1)
    yh, zz, yl, cc, q = src // 128, (src // 16) % 8, (src // 8) % 2, (src // 4) % 2, src % 4
    to = ((cc ^ c) * 128) + ((zz - z) % 8) * 16 + yh * 8 + yl * 4 + q
    return (to == dst).astype(jnp.float32)


def local(a, b):
    x, z, c = lax.axis_index("x"), lax.axis_index("z"), lax.axis_index("c")
    y = lax.axis_index(Y)

    bg = b.reshape(8, 4, 4, 1024)
    b_for = [lax.dynamic_index_in_dim(bg, y ^ d, axis=2, keepdims=False) for d in range(4)]
    b_got = [b_for[0]] + [swap(b_for[d], Y, d) for d in (1, 2, 3)]
    block = jnp.stack([pick(b_got, y ^ k) for k in range(4)], axis=1).reshape(8, 16, 1024)

    ordered = jnp.dot(
        a.reshape(32, 8, 4, 256), lane_order(z, c), precision=lax.Precision.HIGHEST
    )
    a_for = [lax.dynamic_index_in_dim(ordered, x ^ d, axis=2, keepdims=False) for d in range(4)]
    a_got = [a_for[0]] + [swap(a_for[d], "x", d) for d in (1, 2, 3)]
    rows = jnp.stack(a_got)
    near1, near3 = swap(rows, Y, 1), swap(rows, Y, 3)
    far_a, far_b = swap(near3[:2], Y, 1), swap(near1[2:], Y, 3)
    left = jnp.concatenate([rows, near1, far_a, far_b, near3]).reshape(512, 2048)

    mine = [[None] * 8 for _ in range(2)]
    halves = [block[:, :, :512], block[:, :, 512:]]
    for h in range(2):
        mine[h][0] = halves[h]
        up = down = halves[h]
        for s in (1, 2, 3):
            up, down = shift(up, "z", 1), shift(down, "z", -1)
            mine[h][8 - s], mine[h][s] = up, down
        far_up, far_down = shift(up[:, :, :256], "z", 1), shift(down[:, :, 256:], "z", -1)
        mine[h][4] = jnp.concatenate([far_up, far_down], axis=2)
    out = []
    for h in range(2):
        other = [swap(v, "c", 1) for v in mine[h]]
        right = jnp.concatenate(
            [v[:, None] for v in mine[h]] + [v[:, None] for v in other], axis=1
        ).reshape(2048, 512)
        out.append(
            jnp.dot(
                left, right, precision=lax.Precision.HIGH, preferred_element_type=jnp.float32
            ).reshape(4, 4, 32, 512)
        )

    own = []
    for p, first, second in ((out[0], 1, 3), (out[1], 3, 1)):
        got = swap(jnp.stack([p[:, first], p[:, 2]]), "x", first)
        keep, pass_on = p[:, 0] + got[0], p[:, second] + got[1]
        own.append(keep + swap(pass_on, "x", second))
    summed = jnp.concatenate(own, axis=2)
    back = [summed[0]] + [swap(summed[d], Y, d) for d in (1, 2, 3)]
    placed = jnp.stack([pick(back, y ^ k) for k in range(4)], axis=1)
    return placed.reshape(8, 4, 2, 4, 512)


def solution(mesh):
    split = Mesh(mesh.devices.reshape(4, 2, 8, 2, 2), AXES)
    spec = P(None, AXES, None, None, None)
    return jax.shard_map(local, mesh=split, in_specs=(spec, spec), out_specs=spec, check_vma=False)
```

```python
import jax
import jax.numpy as jnp
from jax import lax
from jax.experimental import pallas as pl
from jax.experimental.pallas import tpu as pltpu
from jax.sharding import Mesh
from jax.sharding import PartitionSpec as P

AXES = ("x", "yh", "z", "yl", "c")
Y = ("yh", "yl")
F32, BF16 = jnp.float32, jnp.bfloat16


def swap(v, axis, bits):
    n = lax.axis_size(axis)
    return lax.ppermute(v, axis, [(i, i ^ bits) for i in range(n)])


def shift(v, axis, step):
    n = lax.axis_size(axis)
    return lax.ppermute(v, axis, [(i, (i + step) % n) for i in range(n)])


def pick(pieces, index):
    low = jnp.where(index % 2 == 1, pieces[1], pieces[0])
    high = jnp.where(index % 2 == 1, pieces[3], pieces[2])
    return jnp.where(index >= 2, high, low)


def lane_order(z, c):
    src = lax.broadcasted_iota(jnp.int32, (256, 256), 0)
    dst = lax.broadcasted_iota(jnp.int32, (256, 256), 1)
    yh, zz, yl, cc, q = src // 128, (src // 16) % 8, (src // 8) % 2, (src // 4) % 2, src % 4
    to = ((cc ^ c) * 128) + ((zz - z) % 8) * 16 + yh * 8 + yl * 4 + q
    return (to == dst).astype(F32)


def parts(v):
    high = v.astype(BF16)
    return high, (v - high.astype(F32)).astype(BF16)


def split_left(left):
    n = len(left)

    def kernel(*refs):
        high_ref, low_ref = refs[n:]

        def step(b, carry):
            at = pl.ds(pl.multiple_of(b * 256, 256), 256)
            for g in range(n):
                for d in range(2):
                    rows = pl.ds(64 * g + 32 * d, 32)
                    high_ref[rows, at], low_ref[rows, at] = parts(refs[g][d, b])
            return carry

        lax.fori_loop(0, 8, step, 0)

    return pl.pallas_call(
        kernel,
        out_shape=(jax.ShapeDtypeStruct((64 * n, 2048), BF16),) * 2,
        in_specs=[pl.BlockSpec(memory_space=pltpu.VMEM)] * n,
        out_specs=(pl.BlockSpec(memory_space=pltpu.VMEM),) * 2,
        compiler_params=pltpu.CompilerParams(vmem_limit_bytes=40 * 1024 * 1024),
        name="split_left",
    )(*left)


def product(left, right):
    arrays = []
    for v, _ in right:
        if not any(v is w for w in arrays):
            arrays.append(v)
    where = [(next(k for k, w in enumerate(arrays) if w is v), i) for v, i in right]
    n = len(arrays)

    def kernel(ah, al, *refs):
        o_ref, bh, bl = refs[n:]

        def split(b, carry):
            for k, (r, i) in enumerate(where):
                at = pl.ds(pl.multiple_of(b * 256 + k * 16, 16), 16)
                bh[at, :], bl[at, :] = parts(refs[r][i, b])
            return carry

        lax.fori_loop(0, 8, split, 0)

        def rows(m, carry):
            at = pl.ds(pl.multiple_of(m * 128, 128), 128)
            total = jnp.dot(ah[at, :], bh[...], preferred_element_type=F32)
            total += jnp.dot(ah[at, :], bl[...], preferred_element_type=F32)
            total += jnp.dot(al[at, :], bh[...], preferred_element_type=F32)
            o_ref[at, :] = total
            return carry

        lax.fori_loop(0, 4, rows, 0)

    return pl.pallas_call(
        kernel,
        out_shape=jax.ShapeDtypeStruct((512, 512), F32),
        in_specs=[pl.BlockSpec(memory_space=pltpu.VMEM)] * (n + 2),
        out_specs=pl.BlockSpec(memory_space=pltpu.VMEM),
        scratch_shapes=[pltpu.VMEM((2048, 512), BF16)] * 2,
        compiler_params=pltpu.CompilerParams(vmem_limit_bytes=40 * 1024 * 1024),
        name="product",
    )(*left, *arrays)


def placed_product(a, b):
    x, z, c = lax.axis_index("x"), lax.axis_index("z"), lax.axis_index("c")
    y = lax.axis_index(Y)

    bg = b.reshape(8, 4, 4, 1024)
    b_for = [lax.dynamic_index_in_dim(bg, y ^ d, axis=2, keepdims=False) for d in range(4)]
    b_got = [b_for[0]] + [swap(b_for[d], Y, d) for d in (1, 2, 3)]
    block = jnp.stack([pick(b_got, y ^ k) for k in range(4)], axis=1).reshape(8, 16, 1024)
    halves = [block[:, :, :512], block[:, :, 512:]]

    ordered = jnp.dot(a.reshape(32, 8, 4, 256), lane_order(z, c), precision=lax.Precision.HIGHEST)
    ordered = jnp.transpose(ordered, (2, 1, 0, 3))
    a_for = [lax.dynamic_index_in_dim(ordered, x ^ d, axis=0, keepdims=False) for d in range(4)]
    a_got = [a_for[0]] + [swap(a_for[d], "x", d) for d in (1, 2, 3)]
    low, high = jnp.stack(a_got[:2]), jnp.stack(a_got[2:])
    near3_low, near1_high = swap(low, Y, 3), swap(high, Y, 1)
    near1_low, near3_high = swap(low, Y, 1), swap(high, Y, 3)
    far_low, far_high = swap(near3_low, Y, 1), swap(near1_high, Y, 3)
    left = split_left([low, high, near1_low, near1_high, far_low, far_high, near3_low, near3_high])

    own, other = [{}, {}], [{}, {}]
    both = jnp.stack(halves)
    crossed = swap(both, "c", 1)
    up, down = list(halves), list(halves)
    for h in range(2):
        own[h][0], other[h][0] = (both, h), (crossed, h)
    for s in (1, 2, 3):
        for h in range(2):
            up[h] = shift(up[h], "z", 1)
            down[h] = shift(down[h], "z", -1)
        both = jnp.stack([up[0], down[0], up[1], down[1]])
        crossed = swap(both, "c", 1)
        for h in range(2):
            for i, at in ((2 * h, 8 - s), (2 * h + 1, s)):
                own[h][at], other[h][at] = (both, i), (crossed, i)
    last = [shift(up[0], "z", 1), shift(down[1], "z", -1)]
    for h in range(2):
        crossed = swap(last[h], "c", 1)
        own[h][4], other[h][4] = (last[h][None], 0), (crossed[None], 0)
    out = [
        product(left, [own[h][s] for s in range(8)] + [other[h][s] for s in range(8)]).reshape(4, 4, 32, 512)
        for h in range(2)
    ]

    sums = []
    for p, first, second in ((out[0], 1, 3), (out[1], 3, 1)):
        got = swap(jnp.stack([p[:, first], p[:, 2]]), "x", first)
        keep, pass_on = p[:, 0] + got[0], p[:, second] + got[1]
        sums.append(keep + swap(pass_on, "x", second))
    summed = jnp.concatenate(sums, axis=2)
    back = [summed[0]] + [swap(summed[d], Y, d) for d in (1, 2, 3)]
    placed = jnp.stack([pick(back, y ^ k) for k in range(4)], axis=1)
    return placed.reshape(8, 4, 2, 4, 512)


def solution(mesh):
    split = Mesh(mesh.devices.reshape(4, 2, 8, 2, 2), AXES)
    spec = P(None, AXES, None, None, None)
    return jax.shard_map(placed_product, mesh=split, in_specs=(spec, spec), out_specs=spec, check_vma=False)
```

```python
import jax
import jax.numpy as jnp
from jax import lax
from jax.experimental import pallas as pl
from jax.experimental.pallas import tpu as pltpu
from jax.sharding import Mesh
from jax.sharding import PartitionSpec as P

AXES = ("x", "yh", "z", "yl", "c")
Y = ("yh", "yl")
F32, BF16 = jnp.float32, jnp.bfloat16


EARLY, LATE = (0, 7, 1, 6), (2, 5, 3, 4)

WAYS = ((1, 3), (3, 1))


def swap(v, axis, bits):
    n = lax.axis_size(axis)
    return lax.ppermute(v, axis, [(i, i ^ bits) for i in range(n)])


def shift(v, axis, step):
    n = lax.axis_size(axis)
    return lax.ppermute(v, axis, [(i, (i + step) % n) for i in range(n)])


def pick(pieces, index):
    low = jnp.where(index % 2 == 1, pieces[1], pieces[0])
    high = jnp.where(index % 2 == 1, pieces[3], pieces[2])
    return jnp.where(index >= 2, high, low)


def lane_order(z, c):
    src = lax.broadcasted_iota(jnp.int32, (256, 256), 0)
    dst = lax.broadcasted_iota(jnp.int32, (256, 256), 1)
    yh, zz, yl, cc, q = src // 128, (src // 16) % 8, (src // 8) % 2, (src // 4) % 2, src % 4
    apart = (zz - z) % 8
    place = sum(jnp.where(apart == s, k, 0) for k, s in enumerate(EARLY + LATE))
    to = (place // 4) * 128 + (cc ^ c) * 64 + (place % 4) * 16 + yh * 8 + yl * 4 + q
    return (to == dst).astype(F32)


def parts(v):
    high = v.astype(BF16)
    return high, (v - high.astype(F32)).astype(BF16)


VMEM = pl.BlockSpec(memory_space=pltpu.VMEM)
PARAMS = pltpu.CompilerParams(vmem_limit_bytes=16 * 1024 * 1024)


def column_group():
    return 2 * lax.axis_index("yh") + lax.axis_index("yl")


def cut_right(b):
    def kernel(b_ref, *outs):
        y = column_group()
        for d, out in enumerate(outs):
            k = jnp.bitwise_xor(y, d)
            for i in range(2):
                low, high = b_ref[:, :, k // 2, i, :], b_ref[:, :, k // 2, 2 + i, :]
                out[:, :, pl.ds(512 * i, 512)] = jnp.where(k % 2 == 1, high, low)

    return pl.pallas_call(
        kernel,
        out_shape=(jax.ShapeDtypeStruct((8, 4, 1024), F32),) * 4,
        in_specs=[VMEM],
        out_specs=(VMEM,) * 4,
        compiler_params=PARAMS,
        name="cut_right",
    )(b)


def join_right(got):
    def kernel(*refs):
        y = column_group()
        for k in range(4):
            d = jnp.bitwise_xor(y, k)
            for h in range(2):
                at = pl.ds(512 * h, 512)
                low = jnp.where(d % 2 == 1, refs[1][:, :, at], refs[0][:, :, at])
                high = jnp.where(d % 2 == 1, refs[3][:, :, at], refs[2][:, :, at])
                refs[4 + h][:, pl.ds(4 * k, 4), :] = jnp.where(d >= 2, high, low)

    return pl.pallas_call(
        kernel,
        out_shape=(jax.ShapeDtypeStruct((8, 16, 512), F32),) * 2,
        in_specs=[VMEM] * 4,
        out_specs=(VMEM,) * 2,
        compiler_params=PARAMS,
        name="join_right",
    )(*got)


def split_left(left):
    n = len(left)
    which = [(g, d) for g in range(n) for d in range(left[g].shape[0])]

    def kernel(*refs):
        outs = refs[n:]

        def step(b, carry):
            for k, (g, d) in enumerate(which):
                rows = pl.ds(32 * k, 32)
                for phase in range(2):
                    high, low = parts(refs[g][d, b, :, pl.ds(128 * phase, 128)])
                    for k3, v in enumerate((high, high, low)):
                        at = pl.ds(pl.multiple_of(1024 * k3 + b * 128, 128), 128)
                        outs[phase][rows, at] = v
            return carry

        lax.fori_loop(0, 8, step, 0)

    return pl.pallas_call(
        kernel,
        out_shape=(jax.ShapeDtypeStruct((32 * len(which), 3072), BF16),) * 2,
        in_specs=[VMEM] * n,
        out_specs=(VMEM,) * 2,
        compiler_params=PARAMS,
        name="split_left",
    )(*left)


def sources(blocks):
    arrays = []
    for v, _ in blocks:
        if not any(v is w for w in arrays):
            arrays.append(v)
    return arrays, [(next(k for k, w in enumerate(arrays) if w is v), i) for v, i in blocks]


def stack_right(to, where, refs, b, column=0):
    for k, (r, i) in enumerate(where):
        high, low = parts(refs[r][i, b])
        for k3, v in enumerate((high, low, high)):
            at = pl.ds(pl.multiple_of(1024 * k3 + b * 128 + k * 16, 16), 16)
            to[at, pl.ds(column, 512)] = v


def product(left, right):
    return jnp.dot(left, right, preferred_element_type=F32)


def early_product(left, blocks):
    arrays, where = sources(blocks[0] + blocks[1])
    n = len(arrays)

    def kernel(a, *refs):
        o_ref, right = refs[n:]

        def split(b, carry):
            for h in range(2):
                stack_right(right, where[8 * h : 8 * h + 8], refs, b, 512 * h)
            return carry

        lax.fori_loop(0, 8, split, 0)

        def columns(h, carry):
            at = pl.ds(pl.multiple_of(512 * h, 512), 512)
            o_ref[:, at] = product(a[...], right[:, at])
            return carry

        lax.fori_loop(0, 2, columns, 0)

    return pl.pallas_call(
        kernel,
        out_shape=(
            jax.ShapeDtypeStruct((384, 1024), F32),
            jax.ShapeDtypeStruct((3072, 1024), BF16),
        ),
        in_specs=[VMEM] * (n + 1),
        out_specs=(VMEM,) * 2,
        compiler_params=PARAMS,
        name="early_product",
    )(left, *arrays)


def late_product(near, far, early, blocks, half):
    arrays, where = sources(blocks)
    n = len(arrays)

    def kernel(a, far_early, far_late, total_ref, right_early, *refs):
        outs, right = refs[n : n + 6], refs[n + 6]

        def split(b, carry):
            stack_right(right, where, refs, b)
            return carry

        lax.fori_loop(0, 8, split, 0)
        columns = pl.ds(512 * half, 512)

        def put(slot, total):
            for quarter, (first, second) in enumerate(WAYS):
                keep_ref, pass_ref, send_ref = outs[3 * quarter : 3 * quarter + 3]
                part = total[:, 256 * quarter : 256 * quarter + 256]
                keep_ref[slot] = part[0:32]
                pass_ref[slot] = part[32 * second : 32 * second + 32]
                send_ref[0, slot] = part[32 * first : 32 * first + 32]
                send_ref[1, slot] = part[64:96]

        near_total = product(a[...], right[...]) + total_ref[:, columns]
        for m, slot in enumerate((0, 1, 3)):
            put(slot, near_total[128 * m : 128 * m + 128])
        put(2, product(far_early[...], right_early[:, columns]) + product(far_late[...], right[...]))

    one, two = jax.ShapeDtypeStruct((4, 32, 256), F32), jax.ShapeDtypeStruct((2, 4, 32, 256), F32)
    return pl.pallas_call(
        kernel,
        out_shape=(one, one, two) * 2,
        in_specs=[VMEM] * (n + 5),
        out_specs=(VMEM,) * 6,
        scratch_shapes=[pltpu.VMEM((3072, 512), BF16)],
        compiler_params=PARAMS,
        name="late_product",
    )(near[1], *far, *early, *arrays)


def placed_product(a, b):
    x, z, c = lax.axis_index("x"), lax.axis_index("z"), lax.axis_index("c")
    y = lax.axis_index(Y)

    b_for = cut_right(b)
    b_got = [b_for[0]] + [swap(b_for[d], Y, d) for d in (1, 2, 3)]
    halves = join_right(b_got)

    ordered = jnp.dot(a.reshape(32, 8, 4, 256), lane_order(z, c), precision=lax.Precision.HIGH)
    ordered = jnp.transpose(ordered, (2, 1, 0, 3))
    a_for = [lax.dynamic_index_in_dim(ordered, x ^ d, axis=0, keepdims=False) for d in range(4)]
    a_got = [a_for[0]] + [swap(a_for[d], "x", d) for d in (1, 2, 3)]
    one, rest = a_got[0], jnp.stack(a_got[1:])
    near1 = swap(one, Y, 1), swap(rest, Y, 1)
    near3 = swap(one, Y, 3), swap(rest, Y, 3)
    far_low = swap(jnp.stack([near3[0], near3[1][0]]), Y, 1)
    far_high = swap(near1[1][1:], Y, 3)
    near = split_left([one[None], rest, near1[0][None], near1[1], near3[0][None], near3[1]])
    far = split_left([far_low, far_high])

    own, other = [{}, {}], [{}, {}]
    up, down, held = list(halves), list(halves), list(halves)
    places = [(0, 0), (1, 0)]
    for s in (1, 2, 3):
        for h in range(2):
            up[h] = shift(up[h], "z", 1)
            down[h] = shift(down[h], "z", -1)
        held += [up[0], down[0], up[1], down[1]]
        places += [(0, 8 - s), (0, s), (1, 8 - s), (1, s)]
        if s == 3:
            break
        both = jnp.stack(held)
        crossed = swap(both, "c", 1)
        for i, (h, at) in enumerate(places):
            own[h][at], other[h][at] = (both, i), (crossed, i)
        held, places = [], []
    early = early_product(
        near[0], [[v[h][s] for v in (own, other) for s in EARLY] for h in range(2)]
    )
    held += [shift(up[0], "z", 1), shift(down[1], "z", -1)]
    places += [(0, 4), (1, 4)]
    both = jnp.stack(held)
    crossed = swap(both, "c", 1)
    for i, (h, at) in enumerate(places):
        own[h][at], other[h][at] = (both, i), (crossed, i)

    sums = []
    for h in range(2):
        blocks = [v[h][s] for v in (own, other) for s in LATE]
        pieces = late_product(near, far, early, blocks, h)
        for quarter, (first, second) in enumerate(WAYS):
            keep, pass_on, send = pieces[3 * quarter : 3 * quarter + 3]
            got = swap(send, "x", first)
            sums.append(keep + got[0] + swap(pass_on + got[1], "x", second))
    summed = jnp.concatenate(sums, axis=2)
    back = [summed[0]] + [swap(summed[d], Y, d) for d in (1, 2, 3)]
    placed = jnp.stack([pick(back, y ^ k) for k in range(4)], axis=1)
    return placed.reshape(8, 4, 2, 4, 512)


def solution(mesh):
    split = Mesh(mesh.devices.reshape(4, 2, 8, 2, 2), AXES)
    spec = P(None, AXES, None, None, None)
    return jax.shard_map(placed_product, mesh=split, in_specs=(spec, spec), out_specs=spec, check_vma=False)
```

```python
import jax
import jax.numpy as jnp
from jax import lax
from jax.experimental import pallas as pl
from jax.experimental.pallas import tpu as pltpu
from jax.sharding import Mesh
from jax.sharding import PartitionSpec as P

AXES = ("x", "yh", "z", "yl", "c")
Y = ("yh", "yl")
F32, BF16 = jnp.float32, jnp.bfloat16


EARLY, LATE = (0, 7, 1, 6), (2, 5, 3, 4)

WAYS = ((1, 3), (3, 1))


def swap(v, axis, bits):
    n = lax.axis_size(axis)
    return lax.ppermute(v, axis, [(i, i ^ bits) for i in range(n)])


def shift(v, axis, step):
    n = lax.axis_size(axis)
    return lax.ppermute(v, axis, [(i, (i + step) % n) for i in range(n)])


def lane_order(z, c):
    src = lax.broadcasted_iota(jnp.int32, (256, 256), 0)
    dst = lax.broadcasted_iota(jnp.int32, (256, 256), 1)
    yh, zz, yl, cc, q = src // 128, (src // 16) % 8, (src // 8) % 2, (src // 4) % 2, src % 4
    apart = (zz - z) % 8
    place = sum(jnp.where(apart == s, k, 0) for k, s in enumerate(EARLY + LATE))
    to = (place // 4) * 128 + (cc ^ c) * 64 + (place % 4) * 16 + yh * 8 + yl * 4 + q
    return (to == dst).astype(F32)


def parts(v):
    high = v.astype(BF16)
    return high, (v - high.astype(F32)).astype(BF16)


VMEM = pl.BlockSpec(memory_space=pltpu.VMEM)
PARAMS = pltpu.CompilerParams(vmem_limit_bytes=16 * 1024 * 1024)


def column_group():
    return 2 * lax.axis_index("yh") + lax.axis_index("yl")


def cut_right(b):
    def kernel(b_ref, *outs):
        y = column_group()
        for d, out in enumerate(outs):
            k = jnp.bitwise_xor(y, d)
            for i in range(2):
                low, high = b_ref[:, :, k // 2, i, :], b_ref[:, :, k // 2, 2 + i, :]
                out[:, :, pl.ds(512 * i, 512)] = jnp.where(k % 2 == 1, high, low)

    return pl.pallas_call(
        kernel,
        out_shape=(jax.ShapeDtypeStruct((8, 4, 1024), F32),) * 4,
        in_specs=[VMEM],
        out_specs=(VMEM,) * 4,
        compiler_params=PARAMS,
        cost_estimate=pl.CostEstimate(flops=1<<31, bytes_accessed=1<<23, transcendentals=0),
        name="cut_right",
    )(b)


def place(got):
    def kernel(*refs):
        y = column_group()
        for h in range(2):
            for c in range(4):
                d = jnp.bitwise_xor(y, 2 * h + c // 2)
                at = pl.ds(512 * (c % 2), 512)
                low = jnp.where(d % 2 == 1, refs[1][:, at], refs[0][:, at])
                high = jnp.where(d % 2 == 1, refs[3][:, at], refs[2][:, at])
                refs[4][:, :, h, c, :] = jnp.where(d >= 2, high, low).reshape(8, 4, 512)

    return pl.pallas_call(
        kernel,
        out_shape=jax.ShapeDtypeStruct((8, 4, 2, 4, 512), F32),
        in_specs=[VMEM] * 4,
        compiler_params=PARAMS,
        name="place",
    )(*got)


def join_right(got):
    def kernel(*refs):
        y = column_group()
        for k in range(4):
            d = jnp.bitwise_xor(y, k)
            for h in range(2):
                at = pl.ds(512 * h, 512)
                low = jnp.where(d % 2 == 1, refs[1][:, :, at], refs[0][:, :, at])
                high = jnp.where(d % 2 == 1, refs[3][:, :, at], refs[2][:, :, at])
                refs[4 + h][:, pl.ds(4 * k, 4), :] = jnp.where(d >= 2, high, low)

    return pl.pallas_call(
        kernel,
        out_shape=(jax.ShapeDtypeStruct((8, 16, 512), F32),) * 2,
        in_specs=[VMEM] * 4,
        out_specs=(VMEM,) * 2,
        compiler_params=PARAMS,
        name="join_right",
    )(*got)


def split_left(left):
    n = len(left)
    which = [(g, d) for g in range(n) for d in range(left[g].shape[0])]

    def kernel(*refs):
        outs = refs[n:]

        def step(b, carry):
            for k, (g, d) in enumerate(which):
                rows = pl.ds(32 * k, 32)
                for phase in range(2):
                    high, low = parts(refs[g][d, b, :, pl.ds(128 * phase, 128)])
                    for k3, v in enumerate((high, high, low)):
                        at = pl.ds(pl.multiple_of(1024 * k3 + b * 128, 128), 128)
                        outs[phase][rows, at] = v
            return carry

        lax.fori_loop(0, 8, step, 0)

    return pl.pallas_call(
        kernel,
        out_shape=(jax.ShapeDtypeStruct((32 * len(which), 3072), BF16),) * 2,
        in_specs=[VMEM] * n,
        out_specs=(VMEM,) * 2,
        compiler_params=PARAMS,
        name="split_left",
    )(*left)


def split_far(one, low, high):
    def kernel(one_ref, low_ref, high_ref, *outs):
        def step(b, carry):
            blocks = one_ref[b], low_ref[b], high_ref[b + 4]
            for row, block in zip((0, 32, 96), blocks):
                put(outs, row, b, block)
            return carry

        def put(outs, row, b, block):
            for phase in range(2):
                high, low = parts(block[:, 128 * phase : 128 * phase + 128])
                for k3, v in enumerate((high, high, low)):
                    at = pl.ds(pl.multiple_of(1024 * k3 + b * 128, 128), 128)
                    outs[phase][pl.ds(row, 32), at] = v

        def middle(b, carry):
            put(outs, 64, b, low_ref[b + 8])
            put(outs, 64, b + 4, high_ref[b])
            return carry

        lax.fori_loop(0, 8, step, 0)
        lax.fori_loop(0, 4, middle, 0)

    return pl.pallas_call(
        kernel,
        out_shape=(jax.ShapeDtypeStruct((128, 3072), BF16),) * 2,
        in_specs=[VMEM] * 3,
        out_specs=(VMEM,) * 2,
        compiler_params=PARAMS,
        name="split_far",
    )(one, low, high)


def sources(blocks):
    arrays = []
    for v, _ in blocks:
        if not any(v is w for w in arrays):
            arrays.append(v)
    return arrays, [(next(k for k, w in enumerate(arrays) if w is v), i) for v, i in blocks]


def stack_right(to, where, refs, b, column=0):
    for k, (r, i) in enumerate(where):
        high, low = parts(refs[r][i, b])
        for k3, v in enumerate((high, low, high)):
            at = pl.ds(pl.multiple_of(1024 * k3 + b * 128 + k * 16, 16), 16)
            to[at, pl.ds(column, 512)] = v


def product(left, right):
    return jnp.dot(left, right, preferred_element_type=F32)


def early_product(left, blocks):
    arrays, where = sources(blocks[0] + blocks[1])
    n = len(arrays)

    def kernel(a, *refs):
        o_ref, right = refs[n:]

        def split(b, carry):
            for h in range(2):
                stack_right(right, where[8 * h : 8 * h + 8], refs, b, 512 * h)
            return carry

        lax.fori_loop(0, 8, split, 0)

        def columns(h, carry):
            at = pl.ds(pl.multiple_of(512 * h, 512), 512)
            o_ref[:, at] = product(a[...], right[:, at])
            return carry

        lax.fori_loop(0, 2, columns, 0)

    return pl.pallas_call(
        kernel,
        out_shape=(
            jax.ShapeDtypeStruct((384, 1024), F32),
            jax.ShapeDtypeStruct((3072, 1024), BF16),
        ),
        in_specs=[VMEM] * (n + 1),
        out_specs=(VMEM,) * 2,
        compiler_params=PARAMS,
        name="early_product",
    )(left, *arrays)


def late_product(near, far, early, blocks, half):
    arrays, where = sources(blocks)
    n = len(arrays)

    def kernel(a, far_early, far_late, total_ref, right_early, *refs):
        outs, right = refs[n : n + 6], refs[n + 6]

        def split(b, carry):
            stack_right(right, where, refs, b)
            return carry

        lax.fori_loop(0, 8, split, 0)
        columns = pl.ds(512 * half, 512)

        def put(slot, total):
            for quarter, (first, second) in enumerate(WAYS):
                keep_ref, pass_ref, send_ref = outs[3 * quarter : 3 * quarter + 3]
                part = total[:, 256 * quarter : 256 * quarter + 256]
                keep_ref[slot] = part[0:32]
                pass_ref[slot] = part[32 * second : 32 * second + 32]
                send_ref[0, slot] = part[32 * first : 32 * first + 32]
                send_ref[1, slot] = part[64:96]

        near_total = product(a[...], right[...]) + total_ref[:, columns]
        for m, slot in enumerate((0, 1, 3)):
            put(slot, near_total[128 * m : 128 * m + 128])
        put(2, product(far_early[...], right_early[:, columns]) + product(far_late[...], right[...]))

    one, two = jax.ShapeDtypeStruct((4, 32, 256), F32), jax.ShapeDtypeStruct((2, 4, 32, 256), F32)
    return pl.pallas_call(
        kernel,
        out_shape=(one, one, two) * 2,
        in_specs=[VMEM] * (n + 5),
        out_specs=(VMEM,) * 6,
        scratch_shapes=[pltpu.VMEM((3072, 512), BF16)],
        compiler_params=PARAMS,
        name="late_product",
    )(near[1], *far, *early, *arrays)


def placed_product(a, b):
    x, z, c = lax.axis_index("x"), lax.axis_index("z"), lax.axis_index("c")

    b_for = cut_right(b)
    b_got = [b_for[0]] + [swap(b_for[d], Y, d) for d in (1, 2, 3)]
    halves = join_right(b_got)

    ordered = jnp.dot(a.reshape(32, 8, 4, 256), lane_order(z, c), precision=lax.Precision.HIGH)
    ordered = jnp.transpose(ordered, (2, 1, 0, 3))
    a_for = [lax.dynamic_index_in_dim(ordered, x ^ d, axis=0, keepdims=False) for d in range(4)]
    a_got = [a_for[0]] + [swap(a_for[d], "x", d) for d in (1, 2, 3)]
    one, rest = a_got[0], jnp.stack(a_got[1:])
    near1 = swap(one, Y, 1), swap(rest, Y, 1)
    near3 = swap(one, Y, 3), swap(rest, Y, 3)
    far = [
        swap(one, Y, 2), swap(near3[1].reshape(24, 32, 256)[:12], Y, 1), swap(near1[1].reshape(24, 32, 256)[12:], Y, 3)
    ]
    near = split_left([one[None], rest, near1[0][None], near1[1], near3[0][None], near3[1]])
    far = split_far(*far)

    own, other = [{}, {}], [{}, {}]
    up, down, held = list(halves), list(halves), list(halves)
    places = [(0, 0), (1, 0)]
    for s in (1, 2, 3):
        for h in range(2):
            up[h] = shift(up[h], "z", 1)
            down[h] = shift(down[h], "z", -1)
        held += [up[0], down[0], up[1], down[1]]
        places += [(0, 8 - s), (0, s), (1, 8 - s), (1, s)]
        if s == 3:
            break
        both = jnp.stack(held)
        crossed = swap(both, "c", 1)
        for i, (h, at) in enumerate(places):
            own[h][at], other[h][at] = (both, i), (crossed, i)
        held, places = [], []
    early = early_product(
        near[0], [[v[h][s] for v in (own, other) for s in EARLY] for h in range(2)]
    )
    held += [shift(up[0], "z", 1), shift(down[1], "z", -1)]
    places += [(0, 4), (1, 4)]
    both = jnp.stack(held)
    crossed = swap(both, "c", 1)
    for i, (h, at) in enumerate(places):
        own[h][at], other[h][at] = (both, i), (crossed, i)

    sums = []
    for h in range(2):
        blocks = [v[h][s] for v in (own, other) for s in LATE]
        pieces = late_product(near, far, early, blocks, h)
        for quarter, (first, second) in enumerate(WAYS):
            keep, pass_on, send = pieces[3 * quarter : 3 * quarter + 3]
            got = swap(send, "x", first)
            sums.append(keep + got[0] + swap(pass_on + got[1], "x", second))
    summed = jnp.concatenate(sums, axis=2)
    back = [summed[0]] + [swap(summed[d], Y, d) for d in (1, 2, 3)]
    return place(back)


def solution(mesh):
    split = Mesh(mesh.devices.reshape(4, 2, 8, 2, 2), AXES)
    spec = P(None, AXES, None, None, None)
    return jax.shard_map(placed_product, mesh=split, in_specs=(spec, spec), out_specs=spec, check_vma=False)
```

```python
import jax
import jax.numpy as jnp
from jax import lax
from jax.experimental import pallas as pl
from jax.experimental.pallas import tpu as pltpu
from jax.sharding import Mesh
from jax.sharding import PartitionSpec as P

AXES = ("x", "yh", "z", "yl", "c")
Y = ("yh", "yl")
F32, BF16 = jnp.float32, jnp.bfloat16


EARLY, LATE = (0, 7, 1, 6), (2, 5, 3, 4)

WAYS = ((1, 3), (3, 1))


def swap(v, axis, bits):
    n = lax.axis_size(axis)
    return lax.ppermute(v, axis, [(i, i ^ bits) for i in range(n)])


def shift(v, axis, step):
    n = lax.axis_size(axis)
    return lax.ppermute(v, axis, [(i, (i + step) % n) for i in range(n)])


def lane_order(z, c):
    src = lax.broadcasted_iota(jnp.int32, (256, 256), 0)
    dst = lax.broadcasted_iota(jnp.int32, (256, 256), 1)
    yh, zz, yl, cc, q = src // 128, (src // 16) % 8, (src // 8) % 2, (src // 4) % 2, src % 4
    apart = (zz - z) % 8
    place = sum(jnp.where(apart == s, k, 0) for k, s in enumerate(EARLY + LATE))
    to = (place // 4) * 128 + (cc ^ c) * 64 + (place % 4) * 16 + yh * 8 + yl * 4 + q
    return (to == dst).astype(F32)


def parts(v):
    high = v.astype(BF16)
    return high, (v - high.astype(F32)).astype(BF16)


VMEM = pl.BlockSpec(memory_space=pltpu.VMEM)
PARAMS = pltpu.CompilerParams(vmem_limit_bytes=16 * 1024 * 1024)


def column_group():
    return 2 * lax.axis_index("yh") + lax.axis_index("yl")


def cut_right(b):
    def kernel(b_ref, *outs):
        y = column_group()
        for d, out in enumerate(outs):
            k = jnp.bitwise_xor(y, d)
            for i in range(2):
                low, high = b_ref[:, :, k // 2, i, :], b_ref[:, :, k // 2, 2 + i, :]
                out[:, :, pl.ds(512 * i, 512)] = jnp.where(k % 2 == 1, high, low)

    return pl.pallas_call(
        kernel,
        out_shape=(jax.ShapeDtypeStruct((8, 4, 1024), F32),) * 4,
        in_specs=[VMEM],
        out_specs=(VMEM,) * 4,
        compiler_params=PARAMS,
        cost_estimate=pl.CostEstimate(flops=1<<31, bytes_accessed=1<<23, transcendentals=0),
        name="cut_right",
    )(b)


def place(got):
    def kernel(*refs):
        y = column_group()
        for h in range(2):
            for c in range(4):
                d = jnp.bitwise_xor(y, 2 * h + c // 2)
                at = pl.ds(512 * (c % 2), 512)
                low = jnp.where(d % 2 == 1, refs[1][:, at], refs[0][:, at])
                high = jnp.where(d % 2 == 1, refs[3][:, at], refs[2][:, at])
                refs[4][:, :, h, c, :] = jnp.where(d >= 2, high, low).reshape(8, 4, 512)

    return pl.pallas_call(
        kernel,
        out_shape=jax.ShapeDtypeStruct((8, 4, 2, 4, 512), F32),
        in_specs=[VMEM] * 4,
        compiler_params=PARAMS,
        name="place",
    )(*got)


def join_right(got):
    def kernel(*refs):
        y = column_group()
        for k in range(4):
            d = jnp.bitwise_xor(y, k)
            for h in range(2):
                at = pl.ds(512 * h, 512)
                low = jnp.where(d % 2 == 1, refs[1][:, :, at], refs[0][:, :, at])
                high = jnp.where(d % 2 == 1, refs[3][:, :, at], refs[2][:, :, at])
                refs[4 + h][:, pl.ds(4 * k, 4), :] = jnp.where(d >= 2, high, low)

    return pl.pallas_call(
        kernel,
        out_shape=(jax.ShapeDtypeStruct((8, 16, 512), F32),) * 2,
        in_specs=[VMEM] * 4,
        out_specs=(VMEM,) * 2,
        compiler_params=PARAMS,
        name="join_right",
    )(*got)


def split_left(left):
    n = len(left)
    which = [(g, d) for g in range(n) for d in range(left[g].shape[0])]

    def kernel(*refs):
        outs = refs[n:]

        def step(b, carry):
            for k, (g, d) in enumerate(which):
                rows = pl.ds(32 * k, 32)
                for phase in range(2):
                    high, low = parts(refs[g][d, b, :, pl.ds(128 * phase, 128)])
                    for k3, v in enumerate((high, high, low)):
                        at = pl.ds(pl.multiple_of(1024 * k3 + b * 128, 128), 128)
                        outs[phase][rows, at] = v
            return carry

        lax.fori_loop(0, 8, step, 0)

    return pl.pallas_call(
        kernel,
        out_shape=(jax.ShapeDtypeStruct((32 * len(which), 3072), BF16),) * 2,
        in_specs=[VMEM] * n,
        out_specs=(VMEM,) * 2,
        compiler_params=PARAMS,
        name="split_left",
    )(*left)


def sources(blocks):
    arrays = []
    for v, _ in blocks:
        if not any(v is w for w in arrays):
            arrays.append(v)
    return arrays, [(next(k for k, w in enumerate(arrays) if w is v), i) for v, i in blocks]


def stack_right(to, where, refs, b, column=0):
    for k, (r, i) in enumerate(where):
        high, low = parts(refs[r][i, b])
        for k3, v in enumerate((high, low, high)):
            at = pl.ds(pl.multiple_of(1024 * k3 + b * 128 + k * 16, 16), 16)
            to[at, pl.ds(column, 512)] = v


def product(left, right):
    return jnp.dot(left, right, preferred_element_type=F32)


def early_product(left, blocks):
    arrays, where = sources(blocks[0] + blocks[1])
    n = len(arrays)

    def kernel(a, *refs):
        o_ref, right = refs[n:]

        def split(b, carry):
            for h in range(2):
                stack_right(right, where[8 * h : 8 * h + 8], refs, b, 512 * h)
            return carry

        lax.fori_loop(0, 8, split, 0)

        def columns(h, carry):
            at = pl.ds(pl.multiple_of(512 * h, 512), 512)
            o_ref[:, at] = product(a[...], right[:, at])
            return carry

        lax.fori_loop(0, 2, columns, 0)

    return pl.pallas_call(
        kernel,
        out_shape=(
            jax.ShapeDtypeStruct((384, 1024), F32),
            jax.ShapeDtypeStruct((3072, 1024), BF16),
        ),
        in_specs=[VMEM] * (n + 1),
        out_specs=(VMEM,) * 2,
        compiler_params=PARAMS,
        name="early_product",
    )(left, *arrays)


def late_product(near, far, early, blocks, half):
    arrays, where = sources(blocks)
    n = len(arrays)

    def kernel(a, far_early, far_late, total_ref, right_early, *refs):
        outs, right = refs[n : n + 6], refs[n + 6]

        def split(b, carry):
            stack_right(right, where, refs, b)
            return carry

        lax.fori_loop(0, 8, split, 0)
        columns = pl.ds(512 * half, 512)

        def put(slot, total):
            for quarter, (first, second) in enumerate(WAYS):
                keep_ref, pass_ref, send_ref = outs[3 * quarter : 3 * quarter + 3]
                part = total[:, 256 * quarter : 256 * quarter + 256]
                keep_ref[slot] = part[0:32]
                pass_ref[slot] = part[32 * second : 32 * second + 32]
                send_ref[0, slot] = part[32 * first : 32 * first + 32]
                send_ref[1, slot] = part[64:96]

        near_total = product(a[...], right[...]) + total_ref[:, columns]
        for m, slot in enumerate((0, 1, 3)):
            put(slot, near_total[128 * m : 128 * m + 128])
        put(2, product(far_early[...], right_early[:, columns]) + product(far_late[...], right[...]))

    one, two = jax.ShapeDtypeStruct((4, 32, 256), F32), jax.ShapeDtypeStruct((2, 4, 32, 256), F32)
    return pl.pallas_call(
        kernel,
        out_shape=(one, one, two) * 2,
        in_specs=[VMEM] * (n + 5),
        out_specs=(VMEM,) * 6,
        scratch_shapes=[pltpu.VMEM((3072, 512), BF16)],
        compiler_params=PARAMS,
        name="late_product",
    )(near[1], *far, *early, *arrays)


def placed_product(a, b):
    x, z, c = lax.axis_index("x"), lax.axis_index("z"), lax.axis_index("c")

    b_for = cut_right(b)
    b_got = [b_for[0]] + [swap(b_for[d], Y, d) for d in (1, 2, 3)]
    halves = join_right(b_got)

    ordered = jnp.dot(a.reshape(32, 8, 4, 256), lane_order(z, c), precision=lax.Precision.HIGH)
    ordered = jnp.transpose(ordered, (2, 1, 0, 3))
    a_for = [lax.dynamic_index_in_dim(ordered, x ^ d, axis=0, keepdims=False) for d in range(4)]
    a_got = [a_for[0]] + [swap(a_for[d], "x", d) for d in (1, 2, 3)]
    one, rest = a_got[0], jnp.stack(a_got[1:])
    near1 = swap(one, Y, 1), swap(rest, Y, 1)
    near3 = swap(one, Y, 3), swap(rest, Y, 3)
    far_low = swap(jnp.stack([near3[0], near3[1][0]]), Y, 1)
    far_high = swap(near1[1][1:], Y, 3)
    near = split_left([one[None], rest, near1[0][None], near1[1], near3[0][None], near3[1]])
    far = split_left([far_low, far_high])

    own, other = [{}, {}], [{}, {}]
    up, down, held = list(halves), list(halves), list(halves)
    places = [(0, 0), (1, 0)]
    for s in (1, 2, 3):
        for h in range(2):
            up[h] = shift(up[h], "z", 1)
            down[h] = shift(down[h], "z", -1)
        held += [up[0], down[0], up[1], down[1]]
        places += [(0, 8 - s), (0, s), (1, 8 - s), (1, s)]
        if s == 3:
            break
        both = jnp.stack(held)
        crossed = swap(both, "c", 1)
        for i, (h, at) in enumerate(places):
            own[h][at], other[h][at] = (both, i), (crossed, i)
        held, places = [], []
    early = early_product(
        near[0], [[v[h][s] for v in (own, other) for s in EARLY] for h in range(2)]
    )
    held += [shift(up[0], "z", 1), shift(down[1], "z", -1)]
    places += [(0, 4), (1, 4)]
    both = jnp.stack(held)
    crossed = swap(both, "c", 1)
    for i, (h, at) in enumerate(places):
        own[h][at], other[h][at] = (both, i), (crossed, i)

    sums = []
    for h in range(2):
        blocks = [v[h][s] for v in (own, other) for s in LATE]
        pieces = late_product(near, far, early, blocks, h)
        for quarter, (first, second) in enumerate(WAYS):
            keep, pass_on, send = pieces[3 * quarter : 3 * quarter + 3]
            got = swap(send, "x", first)
            sums.append(keep + got[0] + swap(pass_on + got[1], "x", second))
    summed = jnp.concatenate(sums, axis=2)
    back = [summed[0]] + [swap(summed[d], Y, d) for d in (1, 2, 3)]
    return place(back)


def solution(mesh):
    split = Mesh(mesh.devices.reshape(4, 2, 8, 2, 2), AXES)
    spec = P(None, AXES, None, None, None)
    return jax.shard_map(placed_product, mesh=split, in_specs=(spec, spec), out_specs=spec, check_vma=False)
```

```python
import jax
import jax.numpy as jnp
from jax import lax
from jax.experimental import pallas as pl
from jax.experimental.pallas import tpu as pltpu
from jax.sharding import Mesh
from jax.sharding import PartitionSpec as P

AXES = ("x", "yh", "z", "yl", "c")
Y = ("yh", "yl")
F32, BF16 = jnp.float32, jnp.bfloat16


EARLY, LATE = (0, 7, 1, 6), (2, 5, 3, 4)

WAYS = ((1, 3), (3, 1))


def swap(v, axis, bits):
    n = lax.axis_size(axis)
    return lax.ppermute(v, axis, [(i, i ^ bits) for i in range(n)])


def shift(v, axis, step):
    n = lax.axis_size(axis)
    return lax.ppermute(v, axis, [(i, (i + step) % n) for i in range(n)])


def lane_order(z, c):
    src = lax.broadcasted_iota(jnp.int32, (256, 256), 0)
    dst = lax.broadcasted_iota(jnp.int32, (256, 256), 1)
    yh, zz, yl, cc, q = src // 128, (src // 16) % 8, (src // 8) % 2, (src // 4) % 2, src % 4
    apart = (zz - z) % 8
    place = sum(jnp.where(apart == s, k, 0) for k, s in enumerate(EARLY + LATE))
    to = (place // 4) * 128 + (cc ^ c) * 64 + (place % 4) * 16 + yh * 8 + yl * 4 + q
    return (to == dst).astype(F32)


def parts(v):
    high = v.astype(BF16)
    return high, (v - high.astype(F32)).astype(BF16)


VMEM = pl.BlockSpec(memory_space=pltpu.VMEM)
PARAMS = pltpu.CompilerParams(vmem_limit_bytes=16 * 1024 * 1024)


def column_group():
    return 2 * lax.axis_index("yh") + lax.axis_index("yl")


def cut_right(b):
    def kernel(b_ref, *outs):
        y = column_group()
        for d, out in enumerate(outs):
            k = jnp.bitwise_xor(y, d)
            for i in range(2):
                low, high = b_ref[:, :, k // 2, i, :], b_ref[:, :, k // 2, 2 + i, :]
                out[:, :, pl.ds(512 * i, 512)] = jnp.where(k % 2 == 1, high, low)

    return pl.pallas_call(
        kernel,
        out_shape=(jax.ShapeDtypeStruct((8, 4, 1024), F32),) * 4,
        in_specs=[VMEM],
        out_specs=(VMEM,) * 4,
        compiler_params=PARAMS,
        cost_estimate=pl.CostEstimate(flops=1<<31, bytes_accessed=1<<23, transcendentals=0),
        name="cut_right",
    )(b)


def place(got):
    def kernel(*refs):
        y = column_group()
        for h in range(2):
            for c in range(4):
                d = jnp.bitwise_xor(y, 2 * h + c // 2)
                at = pl.ds(512 * (c % 2), 512)
                low = jnp.where(d % 2 == 1, refs[1][:, at], refs[0][:, at])
                high = jnp.where(d % 2 == 1, refs[3][:, at], refs[2][:, at])
                refs[4][:, :, h, c, :] = jnp.where(d >= 2, high, low).reshape(8, 4, 512)

    return pl.pallas_call(
        kernel,
        out_shape=jax.ShapeDtypeStruct((8, 4, 2, 4, 512), F32),
        in_specs=[VMEM] * 4,
        compiler_params=PARAMS,
        name="place",
    )(*got)


def join_right(got):
    def kernel(*refs):
        y = column_group()
        for k in range(4):
            d = jnp.bitwise_xor(y, k)
            for h in range(2):
                at = pl.ds(512 * h, 512)
                low = jnp.where(d % 2 == 1, refs[1][:, :, at], refs[0][:, :, at])
                high = jnp.where(d % 2 == 1, refs[3][:, :, at], refs[2][:, :, at])
                refs[4 + h][:, pl.ds(4 * k, 4), :] = jnp.where(d >= 2, high, low)

    return pl.pallas_call(
        kernel,
        out_shape=(jax.ShapeDtypeStruct((8, 16, 512), F32),) * 2,
        in_specs=[VMEM] * 4,
        out_specs=(VMEM,) * 2,
        compiler_params=PARAMS,
        name="join_right",
    )(*got)


def split_left(left):
    n = len(left)
    which = [(g, d) for g in range(n) for d in range(left[g].shape[0])]

    def kernel(*refs):
        outs = refs[n:]

        def step(b, carry):
            for k, (g, d) in enumerate(which):
                rows = pl.ds(32 * k, 32)
                for phase in range(2):
                    high, low = parts(refs[g][d, b, :, pl.ds(128 * phase, 128)])
                    for k3, v in enumerate((high, high, low)):
                        at = pl.ds(pl.multiple_of(1024 * k3 + b * 128, 128), 128)
                        outs[phase][rows, at] = v
            return carry

        lax.fori_loop(0, 8, step, 0)

    return pl.pallas_call(
        kernel,
        out_shape=(jax.ShapeDtypeStruct((32 * len(which), 3072), BF16),) * 2,
        in_specs=[VMEM] * n,
        out_specs=(VMEM,) * 2,
        compiler_params=PARAMS,
        name="split_left",
    )(*left)


def sources(blocks):
    arrays = []
    for v, _ in blocks:
        if not any(v is w for w in arrays):
            arrays.append(v)
    return arrays, [(next(k for k, w in enumerate(arrays) if w is v), i) for v, i in blocks]


def stack_right(to, where, refs, b, column=0):
    for k, (r, i) in enumerate(where):
        high, low = parts(refs[r][i, b])
        for k3, v in enumerate((high, low, high)):
            at = pl.ds(pl.multiple_of(1024 * k3 + b * 128 + k * 16, 16), 16)
            to[at, pl.ds(column, 512)] = v


def product(left, right):
    return jnp.dot(left, right, preferred_element_type=F32)


def early_product(left, blocks):
    arrays, where = sources(blocks[0] + blocks[1])
    n = len(arrays)

    def kernel(a, *refs):
        o_ref, right = refs[n:]

        def split(b, carry):
            for h in range(2):
                stack_right(right, where[8 * h : 8 * h + 8], refs, b, 512 * h)
            return carry

        lax.fori_loop(0, 8, split, 0)

        def columns(h, carry):
            at = pl.ds(pl.multiple_of(512 * h, 512), 512)
            o_ref[:, at] = product(a[...], right[:, at])
            return carry

        lax.fori_loop(0, 2, columns, 0)

    return pl.pallas_call(
        kernel,
        out_shape=(
            jax.ShapeDtypeStruct((384, 1024), F32),
            jax.ShapeDtypeStruct((3072, 1024), BF16),
        ),
        in_specs=[VMEM] * (n + 1),
        out_specs=(VMEM,) * 2,
        compiler_params=PARAMS,
        name="early_product",
    )(left, *arrays)


def far_product(left, right):
    def kernel(a, b, o_ref):
        o_ref[...] = product(a[...], b[...])

    return pl.pallas_call(
        kernel,
        out_shape=jax.ShapeDtypeStruct((128, 1024), F32),
        in_specs=[VMEM] * 2,
        out_specs=VMEM,
        compiler_params=PARAMS,
        name="far_product",
    )(left, right)


def late_product(near, far, early, blocks, half):
    arrays, where = sources(blocks)
    n = len(arrays)

    def kernel(a, far_late, total_ref, far_ref, *refs):
        outs, right = refs[n : n + 6], refs[n + 6]

        def split(b, carry):
            stack_right(right, where, refs, b)
            return carry

        lax.fori_loop(0, 8, split, 0)
        columns = pl.ds(512 * half, 512)

        def put(slot, total):
            for quarter, (first, second) in enumerate(WAYS):
                keep_ref, pass_ref, send_ref = outs[3 * quarter : 3 * quarter + 3]
                part = total[:, 256 * quarter : 256 * quarter + 256]
                keep_ref[slot] = part[0:32]
                pass_ref[slot] = part[32 * second : 32 * second + 32]
                send_ref[0, slot] = part[32 * first : 32 * first + 32]
                send_ref[1, slot] = part[64:96]

        near_total = product(a[...], right[...]) + total_ref[:, columns]
        for m, slot in enumerate((0, 1, 3)):
            put(slot, near_total[128 * m : 128 * m + 128])
        put(2, product(far_late[...], right[...]) + far_ref[:, columns])

    one, two = jax.ShapeDtypeStruct((4, 32, 256), F32), jax.ShapeDtypeStruct((2, 4, 32, 256), F32)
    return pl.pallas_call(
        kernel,
        out_shape=(one, one, two) * 2,
        in_specs=[VMEM] * (n + 4),
        out_specs=(VMEM,) * 6,
        scratch_shapes=[pltpu.VMEM((3072, 512), BF16)],
        compiler_params=PARAMS,
        name="late_product",
    )(near, far, *early, *arrays)


def placed_product(a, b):
    x, z, c = lax.axis_index("x"), lax.axis_index("z"), lax.axis_index("c")

    b_for = cut_right(b)
    b_got = [b_for[0]] + [swap(b_for[d], Y, d) for d in (1, 2, 3)]
    halves = join_right(b_got)

    ordered = jnp.dot(a.reshape(32, 8, 4, 256), lane_order(z, c), precision=lax.Precision.HIGH)
    ordered = jnp.transpose(ordered, (2, 1, 0, 3))
    a_for = [lax.dynamic_index_in_dim(ordered, x ^ d, axis=0, keepdims=False) for d in range(4)]
    a_got = [a_for[0]] + [swap(a_for[d], "x", d) for d in (1, 2, 3)]
    one, rest = a_got[0], jnp.stack(a_got[1:])
    near1 = swap(one, Y, 1), swap(rest, Y, 1)
    near3 = swap(one, Y, 3), swap(rest, Y, 3)
    far_low = swap(jnp.stack([near3[0], near3[1][0]]), Y, 1)
    far_high = swap(near1[1][1:], Y, 3)
    near = split_left([one[None], rest, near1[0][None], near1[1], near3[0][None], near3[1]])
    far = split_left([far_low, far_high])

    own, other = [{}, {}], [{}, {}]
    up, down, held = list(halves), list(halves), list(halves)
    places = [(0, 0), (1, 0)]
    for s in (1, 2, 3):
        for h in range(2):
            up[h] = shift(up[h], "z", 1)
            down[h] = shift(down[h], "z", -1)
        held += [up[0], down[0], up[1], down[1]]
        places += [(0, 8 - s), (0, s), (1, 8 - s), (1, s)]
        if s == 3:
            break
        both = jnp.stack(held)
        crossed = swap(both, "c", 1)
        for i, (h, at) in enumerate(places):
            own[h][at], other[h][at] = (both, i), (crossed, i)
        held, places = [], []
    early = early_product(
        near[0], [[v[h][s] for v in (own, other) for s in EARLY] for h in range(2)]
    )
    totals = early[0], far_product(far[0], early[1])
    held += [shift(up[0], "z", 1), shift(down[1], "z", -1)]
    places += [(0, 4), (1, 4)]
    both = jnp.stack(held)
    crossed = swap(both, "c", 1)
    for i, (h, at) in enumerate(places):
        own[h][at], other[h][at] = (both, i), (crossed, i)

    sums = []
    for h in range(2):
        blocks = [v[h][s] for v in (own, other) for s in LATE]
        pieces = late_product(near[1], far[1], totals, blocks, h)
        for quarter, (first, second) in enumerate(WAYS):
            keep, pass_on, send = pieces[3 * quarter : 3 * quarter + 3]
            got = swap(send, "x", first)
            sums.append(keep + got[0] + swap(pass_on + got[1], "x", second))
    summed = jnp.concatenate(sums, axis=2)
    back = [summed[0]] + [swap(summed[d], Y, d) for d in (1, 2, 3)]
    return place(back)


def solution(mesh):
    split = Mesh(mesh.devices.reshape(4, 2, 8, 2, 2), AXES)
    spec = P(None, AXES, None, None, None)
    return jax.shard_map(placed_product, mesh=split, in_specs=(spec, spec), out_specs=spec, check_vma=False)
```
